32 devices in a mesh: sp: 16 (over z, y, core), dp: 2 (over x).
Axes of the slice: x: 2, y: 2, z: 4, core: 2. Of those that a mesh axis runs over, the one named last changes fastest.
Arguments:
- query_proj: bfloat16 [4096, 8192], P(('dp', 'sp')), parts along dimension 0, may hold values from -64 to 64
- key_projection: bfloat16 [4096, 1024], P(('dp', 'sp')), parts along dimension 0, may hold values from -64 to 64
- value_projection: bfloat16 [4096, 1024], P(('dp', 'sp')), parts along dimension 0, may hold values from -12 to 12
- query_gain: float32 [128], replicated, may hold values from 1 to 5
- key_norm_gain: float32 [128], replicated, may hold values from 1 to 5
- positions: int32 [4096], P(('dp', 'sp')), parts along dimension 0, may hold values from 0 to 5118, as said below
- doc_start: int32 [4096], P(('dp', 'sp')), parts along dimension 0, may hold values from 0 to 2047, as said below
Outputs:
- attention: bfloat16 [4096, 8192], P(('dp', 'sp')), parts along dimension 0
The draws below stay inside these ranges and needn't reach their ends.
There are 2 independent parts, one for each index of `dp`. The reference program is written for one: setup_inputs(seed, part) draws one part's arguments, and reference() takes and returns one part's arrays. A program takes and returns all parts, laid end to end along the dimension named above; an argument that names none is the same for every part. Nothing has to cross between parts.
Inputs may be any that keep to these rules, and one draw needn't show every extreme that they name: doc_start[i] is the index of the first token of token i's document: it never falls, doc_start[i] <= i < doc_start[i] + 1024, some document has exactly 1024 tokens, and every document but the last has 128 tokens or more. `positions`: within one document the position rises by one from each token to the next.
All inputs are finite; a program needn't handle non-finite values.
Results may differ from the reference program's by a relative error of at most 0.0039.
The reference program's roundings to bfloat16 on the way count: a program that leaves them out, or rounds other values in their place, can miss the bound.
Values may be sent and summed in bfloat16 or wider, within the bound.
A program may use at most 64 MiB of HBM per device.

```python
import jax
import jax.numpy as jnp
from jax import lax

QUERY_HEADS = 64
KEY_VALUE_HEADS = 8
HEAD_SIZE = 128
DOC_MAX = 1024
PACK_TOKENS = 2048


def doc_layout(key):
    rotary_base = jax.random.fold_in(key, 11)
    shortest = DOC_MAX // 8
    count = PACK_TOKENS // shortest + 1
    lengths = jax.random.randint(jax.random.fold_in(rotary_base, 1), (count,), shortest, DOC_MAX + 1, dtype=jnp.int32)
    forced = jax.random.randint(jax.random.fold_in(rotary_base, 2), (), 0, 2, dtype=jnp.int32)
    lengths = jnp.where(jnp.arange(count, dtype=jnp.int32) == forced, DOC_MAX, lengths).astype(jnp.int32)
    starts = (jnp.cumsum(lengths) - lengths).astype(jnp.int32)
    token_index = jnp.arange(PACK_TOKENS, dtype=jnp.int32)
    doc_index = jnp.sum((starts[None, :] <= token_index[:, None]).astype(jnp.int32), axis=1) - 1
    doc_first = starts[doc_index]
    offsets = jax.random.randint(jax.random.fold_in(rotary_base, 3), (count,), 0, 4 * DOC_MAX, dtype=jnp.int32)
    positions = offsets[doc_index] + token_index - doc_first
    return (doc_first.astype(jnp.int32), positions.astype(jnp.int32))


def qk_fields(key):
    rotary_base = jax.random.fold_in(key, 23)
    q_vals = jax.random.normal(jax.random.fold_in(rotary_base, 1), (PACK_TOKENS, QUERY_HEADS, HEAD_SIZE), jnp.float32)
    key_values_local = jax.random.normal(jax.random.fold_in(rotary_base, 2), (PACK_TOKENS, KEY_VALUE_HEADS, HEAD_SIZE), jnp.float32)
    q_vals = jnp.clip(q_vals, -64.0, 64.0).reshape(PACK_TOKENS, QUERY_HEADS * HEAD_SIZE)
    key_values_local = jnp.clip(key_values_local, -64.0, 64.0).reshape(PACK_TOKENS, KEY_VALUE_HEADS * HEAD_SIZE)
    return (q_vals, key_values_local)


def draw_query_proj(key, part):
    return qk_fields(key)[0].astype(jnp.bfloat16)


def draw_key_projection(key, part):
    return qk_fields(key)[1].astype(jnp.bfloat16)


def draw_query_gain(key, part):
    sub_key = jax.random.fold_in(key, 31)
    return jax.random.uniform(sub_key, (HEAD_SIZE,), jnp.float32, 1.0, 2.0)


def draw_key_norm_gain(key, part):
    sub_key = jax.random.fold_in(key, 37)
    return jax.random.uniform(sub_key, (HEAD_SIZE,), jnp.float32, 1.0, 2.0)


def draw_positions(key, part):
    return doc_layout(key)[1]


def draw_doc_start(key, part):
    return doc_layout(key)[0]


def block_levels(rng, dims, pieces, smallest, largest):
    loudness, own = 1.0, jax.random.fold_in(rng, 6)
    for axis_at, blocks in pieces:
        steps = jnp.exp(jax.random.uniform(jax.random.fold_in(own, axis_at), (blocks,), jnp.float32, smallest / len(pieces), largest / len(pieces)))
        loudness = loudness * jnp.repeat(steps, dims[axis_at] // blocks).reshape([-1 if axis == axis_at else 1 for axis in range(len(dims))])
    return loudness


def normal_values(own_key, extent, spread, reach, split=(), held_as=jnp.bfloat16):
    drawn = spread * jax.random.normal(own_key, extent, jnp.float32)
    if split:
        drawn = drawn * block_levels(own_key, extent, split, -0.22, 0.18)
    return jnp.clip(drawn, -reach, reach).astype(held_as)


def setup_inputs(seed: int = 0, part: int = 0) -> dict:
    key_of = jax.random.split(jax.random.key(seed), 8)
    own_keys = jax.random.split(jax.random.fold_in(key_of[7], part), 8)
    return {
        "query_proj": draw_query_proj(jax.random.fold_in(jax.random.fold_in(key_of[7], part), 71), part),
        "key_projection": draw_key_projection(jax.random.fold_in(jax.random.fold_in(key_of[7], part), 71), part),
        "value_projection": normal_values(own_keys[2], (PACK_TOKENS, KEY_VALUE_HEADS * HEAD_SIZE), 2.0, 12.0, ((0, 16),)),
        "query_gain": draw_query_gain(jax.random.fold_in(key_of[7], 71), part),
        "key_norm_gain": draw_key_norm_gain(jax.random.fold_in(key_of[7], 71), part),
        "positions": draw_positions(jax.random.fold_in(jax.random.fold_in(key_of[7], part), 71), part),
        "doc_start": draw_doc_start(jax.random.fold_in(jax.random.fold_in(key_of[7], part), 71), part),
    }


ROPE_BASE = 1000000.0
NORM_EPS = 1e-06

def rotary_tables(positions):
    half_dim = HEAD_SIZE // 2
    inv_freq = ROPE_BASE ** (-(jnp.arange(half_dim, dtype=jnp.float32) * 2.0 / HEAD_SIZE))
    angle = positions.astype(jnp.float32)[:, None] * inv_freq[None, :]
    return (jnp.cos(angle), jnp.sin(angle))

def normalize_and_rotate(heads_in, gain, cosine_table, sine_table):
    upcast = heads_in.astype(jnp.float32)
    mean_square = lax.optimization_barrier(jnp.mean(upcast * upcast, axis=-1, keepdims=True))
    normed = upcast * lax.rsqrt(mean_square + NORM_EPS) * gain
    half_dim = normed.shape[-1] // 2
    first_half = normed[..., :half_dim]
    second_half = normed[..., half_dim:]
    cos_rows = cosine_table[:, None, :]
    sin_rows = sine_table[:, None, :]
    rotated = jnp.concatenate([first_half * cos_rows - second_half * sin_rows, second_half * cos_rows + first_half * sin_rows], axis=-1)
    return rotated.astype(jnp.bfloat16)

def attend(q_head, k_head, v_head, starts):
    rows_all = q_head.shape[0]
    block_rows = min(512, rows_all)
    key_window = DOC_MAX + block_rows
    zero_rows = jnp.zeros((DOC_MAX, q_head.shape[1]), q_head.dtype)
    k_padded = jnp.concatenate([zero_rows, k_head], axis=0)
    v_padded = jnp.concatenate([zero_rows, v_head], axis=0)
    scale = q_head.shape[1] ** (-0.5)

    def one_block(block_index):
        block_start = (block_index * block_rows).astype(jnp.int32)
        query_block = lax.dynamic_slice_in_dim(q_head, block_start, block_rows, 0)
        key_block = lax.dynamic_slice_in_dim(k_padded, block_start, key_window, 0)
        value_block = lax.dynamic_slice_in_dim(v_padded, block_start, key_window, 0)
        doc_first = lax.dynamic_slice_in_dim(starts, block_start, block_rows, 0)
        row_index = block_start + jnp.arange(block_rows, dtype=jnp.int32)
        key_index = block_start - DOC_MAX + jnp.arange(key_window, dtype=jnp.int32)
        visible = (key_index[None, :] >= doc_first[:, None]) & (key_index[None, :] <= row_index[:, None])
        scores = jnp.dot(query_block, key_block.T, preferred_element_type=jnp.float32) * scale
        scores = jnp.where(visible, scores, -jnp.inf)
        row_max = lax.optimization_barrier(jnp.max(scores, axis=1, keepdims=True))
        exp_scores = jnp.exp(scores - row_max)
        row_total = lax.optimization_barrier(jnp.sum(exp_scores, axis=1, keepdims=True))
        weights = exp_scores.astype(jnp.bfloat16)
        mixed_out = jnp.dot(weights, value_block, preferred_element_type=jnp.float32) / row_total
        return mixed_out.astype(jnp.bfloat16)
    blocks = lax.map(one_block, jnp.arange(rows_all // block_rows, dtype=jnp.int32))
    return blocks.reshape(rows_all, q_head.shape[1])

def reference(query_proj, key_projection, value_projection, query_gain, key_norm_gain, positions, doc_start):
    cosine_table, sine_table = rotary_tables(positions)
    q_rope = normalize_and_rotate(query_proj.reshape(PACK_TOKENS, QUERY_HEADS, HEAD_SIZE), query_gain, cosine_table, sine_table)
    key_rotated = normalize_and_rotate(key_projection.reshape(PACK_TOKENS, KEY_VALUE_HEADS, HEAD_SIZE), key_norm_gain, cosine_table, sine_table)
    value_head_split = value_projection.reshape(PACK_TOKENS, KEY_VALUE_HEADS, HEAD_SIZE)
    head_copies = QUERY_HEADS // KEY_VALUE_HEADS
    q_major = jnp.transpose(q_rope, (1, 0, 2))
    k_major = jnp.repeat(jnp.transpose(key_rotated, (1, 0, 2)), head_copies, axis=0)
    v_major = jnp.repeat(jnp.transpose(value_head_split, (1, 0, 2)), head_copies, axis=0)

    def one_head(operands):
        return attend(operands[0], operands[1], operands[2], doc_start)
    per_head = lax.map(one_head, (q_major, k_major, v_major))
    return jnp.transpose(per_head, (1, 0, 2)).reshape(PACK_TOKENS, QUERY_HEADS * HEAD_SIZE)
```

```python
import functools
import math

import jax
import jax.numpy as jnp
import numpy as np
from jax import lax
from jax.experimental import pallas as pl
from jax.experimental.pallas import tpu as pltpu
from jax.sharding import PartitionSpec as P

HEAD_SIZE = 128
DOC_MAX = 1024
REACH = 8
ROPE_BASE = 1000000.0
NORM_EPS = 1e-06
HIDDEN = -1e30
Q_TILE = 2
MESH = pl.DeviceIdType.MESH

OWN_Z, OWN_Y, OWN_C, F4_Z, F4_Y, F4_C, F8_Y, F8_C, F2_C, F6_C = range(10)


def norm_rope(block, gain, cos_full, sin_full):
    up = block.astype(jnp.float32)
    mean_square = jnp.mean(up * up, axis=-1, keepdims=True)
    normed = up * lax.rsqrt(mean_square + NORM_EPS) * gain
    swapped = pltpu.roll(normed, HEAD_SIZE // 2, axis=1)
    return (normed * cos_full + swapped * sin_full).astype(jnp.bfloat16)


def kernel(
    count, groups, copies, rows,
    q_hbm, k_hbm, v_hbm, qg_hbm, kg_hbm, freq_hbm, pos_hbm, start_hbm,
    o_ref, win, hidden, q_ref, k_ref, q_rope, qg_ref, kg_ref, freq_ref, pos_ref, start_ref,
    local_sem, in_sem, send_sem, recv_sem,
):
    me = lax.axis_index("sp")
    core = lax.rem(me, 2)
    side = lax.rem(lax.div(me, 2), 2)
    core_peer = me + 1 - 2 * core
    side_peer = me + 2 - 4 * side
    window = (REACH + 1) * rows

    def slot_rows(slot):
        return pl.ds(pl.multiple_of((REACH - slot) * rows, rows), rows)

    def send(kind, g, source, target_slot, target):
        return pltpu.make_async_remote_copy(
            src_ref=win.at[g, :, slot_rows(source)],
            dst_ref=win.at[g, :, slot_rows(target_slot)],
            send_sem=send_sem.at[kind, g],
            recv_sem=recv_sem.at[target_slot, g],
            device_id={"sp": target},
            device_id_type=MESH,
        )

    has_next = me + 4 < count
    f4_slot = 6 - 4 * side

    plan = {
        OWN_Z: (has_next, 0, 4, me + 4),
        OWN_Y: (side == 0, 0, 2, side_peer),
        OWN_C: (core == 0, 0, 1, core_peer),
        F4_Z: ((me >= 4) & has_next, 4, 8, me + 4),
        F4_Y: (me >= 4, 4, f4_slot, side_peer),
        F4_C: (me >= 4, 4, 5 - 2 * core, core_peer),
        F8_Y: ((me >= 8) & (side == 1), 8, 6, side_peer),
        F8_C: ((me >= 8) & (core == 1), 8, 7, core_peer),
        F2_C: (me >= 2, 2, 3 - 2 * core, core_peer),
        F6_C: (me >= 6, 6, 7 - 2 * core, core_peer),
    }

    def start(kind, g):
        condition, source, target_slot, target = plan[kind]

        @pl.when(condition)
        def _():
            send(kind, g, source, target_slot, target).start()

    def arrived(slot, g):
        @pl.when(me >= slot)
        def _():
            send(OWN_Z, g, 0, slot, me).wait_recv()

    value_copies = [
        pltpu.make_async_copy(
            v_hbm.at[:, pl.ds(g * HEAD_SIZE, HEAD_SIZE)],
            win.at[g, 1, pl.ds(REACH * rows, rows)],
            local_sem.at[g],
        )
        for g in range(groups)
    ]
    small = [
        pltpu.make_async_copy(source, target, in_sem.at[i])
        for i, (source, target) in enumerate([
            (k_hbm, k_ref), (kg_hbm, kg_ref), (freq_hbm, freq_ref), (pos_hbm, pos_ref),
            (start_hbm, start_ref), (qg_hbm, qg_ref),
        ])
    ]
    query_copy = pltpu.make_async_copy(q_hbm, q_ref, in_sem.at[6])
    for copy in small + value_copies + [query_copy]:
        copy.start()
    barrier = pltpu.get_barrier_semaphore()
    for peer in (core_peer, side_peer):
        pl.semaphore_signal(barrier, inc=1, device_id={"sp": peer}, device_id_type=MESH)

    @pl.when(has_next)
    def _():
        pl.semaphore_signal(barrier, inc=1, device_id={"sp": me + 4}, device_id_type=MESH)

    @pl.when(me >= 4)
    def _():
        pl.semaphore_signal(barrier, inc=1, device_id={"sp": me - 4}, device_id_type=MESH)

    for copy in small:
        copy.wait()
    places = jnp.broadcast_to(pos_ref[...].astype(jnp.float32), (HEAD_SIZE, rows)).T
    angle = places * freq_ref[...]
    lane = lax.broadcasted_iota(jnp.int32, (rows, HEAD_SIZE), 1)
    cos_full = jnp.cos(angle)
    sine = jnp.sin(angle)
    sin_full = jnp.where(lane < HEAD_SIZE // 2, -sine, sine)
    for g in range(groups):
        win[g, 0, pl.ds(REACH * rows, rows), :] = norm_rope(
            k_ref[:, g * HEAD_SIZE:(g + 1) * HEAD_SIZE], kg_ref[...], cos_full, sin_full
        )

    token = me * rows + lax.broadcasted_iota(jnp.int32, (window, rows), 1)
    key_index = (me - REACH) * rows + lax.broadcasted_iota(jnp.int32, (window, rows), 0)
    visible = (key_index >= start_ref[...]) & (key_index <= token)
    hidden[...] = jnp.where(visible, 0.0, HIDDEN).astype(jnp.bfloat16)

    @pl.loop(0, jnp.maximum(REACH - me, 0))
    def _(j):
        for g in range(groups):
            win[g, :, pl.ds(pl.multiple_of(j * rows, rows), rows), :] = jnp.zeros(
                (2, rows, HEAD_SIZE), jnp.bfloat16
            )

    for copy in value_copies:
        copy.wait()
    inner = (me >= 4) & has_next

    @pl.when(inner)
    def _():
        pl.semaphore_wait(barrier, 4)

    @pl.when(jnp.logical_not(inner))
    def _():
        pl.semaphore_wait(barrier, 3 if count > 4 else 2)

    scale = HEAD_SIZE ** (-0.5) * math.log2(math.e)

    unit = (
        lax.broadcasted_iota(jnp.int32, (rows, rows), 0)
        == lax.broadcasted_iota(jnp.int32, (rows, rows), 1)
    ).astype(jnp.bfloat16)
    units = jnp.concatenate([unit] * Q_TILE, axis=0)

    def columns(g, head):
        return pl.ds(pl.multiple_of((g * copies + head) * HEAD_SIZE, HEAD_SIZE), HEAD_SIZE)

    def attend(g):
        keys = jnp.concatenate([win[g, 0], hidden[...]], axis=1)
        values = jnp.concatenate(
            [win[g, 1], jnp.ones((window, HEAD_SIZE), jnp.bfloat16)], axis=1
        )
        for first in range(0, copies, Q_TILE):
            queries = jnp.concatenate(
                [q_rope[g, first * rows:(first + Q_TILE) * rows], units], axis=1
            )
            scores = lax.dot_general(
                queries, keys, (((1,), (1,)), ((), ())), preferred_element_type=jnp.float32
            )
            row_max = jnp.max(scores, axis=1, keepdims=True)
            weights = jnp.exp2((scores - row_max) * scale).astype(jnp.bfloat16)
            mixed = jnp.dot(weights, values, preferred_element_type=jnp.float32)
            mixed = mixed[:, :HEAD_SIZE] / mixed[:, HEAD_SIZE:]
            for r in range(Q_TILE):
                o_ref[:, columns(g, first + r)] = mixed[r * rows:(r + 1) * rows].astype(
                    jnp.bfloat16
                )

    LEAD = 4
    for g in range(min(LEAD, groups)):
        for kind in (OWN_Z, OWN_Y, OWN_C):
            start(kind, g)

    query_copy.wait()

    @pl.loop(0, groups)
    def _(g):
        for head in range(copies):
            q_rope[g, head * rows:(head + 1) * rows] = norm_rope(
                q_ref[:, columns(g, head)], qg_ref[...], cos_full, sin_full
            )

    @pl.loop(0, groups + 3)
    def _(tick):
        @pl.when(tick + LEAD < groups)
        def _():
            for kind in (OWN_Z, OWN_Y, OWN_C):
                start(kind, tick + LEAD)

        @pl.when(tick < groups)
        def _():
            arrived(4, tick)
            for kind in (F4_Z, F4_Y, F4_C):
                start(kind, tick)

        @pl.when((tick >= 1) & (tick < groups + 1))
        def _():
            arrived(8, tick - 1)
            for kind in (F8_Y, F8_C):
                start(kind, tick - 1)
            arrived(2, tick - 1)
            start(F2_C, tick - 1)

        @pl.when((tick >= 2) & (tick < groups + 2))
        def _():
            arrived(6, tick - 2)
            start(F6_C, tick - 2)

        @pl.when(tick >= 3)
        def _():
            for slot in (1, 3, 5, 7):
                arrived(slot, tick - 3)
            attend(tick - 3)

    @pl.loop(0, groups)
    def _(g):
        for kind, (condition, source, target_slot, target) in plan.items():
            @pl.when(condition)
            def _():
                send(kind, g, source, target_slot, target).wait_send()


def solution(mesh):
    count = mesh.shape["sp"]

    def body(query_proj, key_projection, value_projection, query_gain, key_norm_gain, positions, doc_start):
        rows = query_proj.shape[0]
        groups = key_projection.shape[1] // HEAD_SIZE
        copies = query_proj.shape[1] // key_projection.shape[1]
        assert rows * REACH >= DOC_MAX and count % 4 == 0
        half_dim = HEAD_SIZE // 2
        inv_freq = ROPE_BASE ** (-(np.arange(half_dim) * 2.0 / HEAD_SIZE))
        freq = jnp.asarray(np.concatenate([inv_freq, inv_freq])[None, :], jnp.float32)
        window = (REACH + 1) * rows
        return pl.pallas_call(
            functools.partial(kernel, count, groups, copies, rows),
            out_shape=jax.ShapeDtypeStruct(query_proj.shape, jnp.bfloat16),
            in_specs=[pl.BlockSpec(memory_space=pl.ANY)] * 8,
            out_specs=pl.BlockSpec(memory_space=pltpu.VMEM),
            scratch_shapes=[
                pltpu.VMEM((groups, 2, window, HEAD_SIZE), jnp.bfloat16),
                pltpu.VMEM((window, rows), jnp.bfloat16),
                pltpu.VMEM(query_proj.shape, jnp.bfloat16),
                pltpu.VMEM(key_projection.shape, jnp.bfloat16),
                pltpu.VMEM((groups, copies * rows, HEAD_SIZE), jnp.bfloat16),
                pltpu.VMEM((1, HEAD_SIZE), jnp.float32),
                pltpu.VMEM((1, HEAD_SIZE), jnp.float32),
                pltpu.VMEM((1, HEAD_SIZE), jnp.float32),
                pltpu.VMEM((1, rows), jnp.int32),
                pltpu.VMEM((1, rows), jnp.int32),
                pltpu.SemaphoreType.DMA((groups,)),
                pltpu.SemaphoreType.DMA((7,)),
                pltpu.SemaphoreType.DMA((10, groups)),
                pltpu.SemaphoreType.DMA((REACH + 1, groups)),
            ],
            compiler_params=pltpu.CompilerParams(
                collective_id=0, has_side_effects=True, vmem_limit_bytes=60 * 1024 * 1024
            ),
        )(
            query_proj, key_projection, value_projection,
            query_gain[None, :], key_norm_gain[None, :], freq, positions[None, :], doc_start[None, :],
        )

    tokens = P(("dp", "sp"), None)
    vector = P(("dp", "sp"))
    return jax.shard_map(
        body,
        mesh=mesh,
        in_specs=(tokens, tokens, tokens, P(), P(), vector, vector),
        out_specs=tokens,
        check_vma=False,
    )
```
